256 devices in a mesh: seq: 32 (over y_lo, z, core), head: 8 (over x, y_hi).
Axes of the slice: x: 4, y: 4 (y_hi: 2, y_lo: 2; y = y_hi * 2 + y_lo), z: 8, core: 2. Of those that a mesh axis runs over, the one named last changes fastest.
Arguments:
- queries: bfloat16 [4, 64, 64, 128], P(None, None, 'head'), may hold values from -15 to 15
- new_keys: bfloat16 [4, 64, 8, 128], P(None, None, 'head'), may hold values from -16 to 16
- new_values: bfloat16 [4, 64, 8, 128], P(None, None, 'head'), may hold values from -6 to 6
- cache_keys: bfloat16 [4, 65536, 8, 128], P(None, 'seq', 'head'), may hold values from -6 to 6
- cache_values: bfloat16 [4, 65536, 8, 128], P(None, 'seq', 'head'), may hold values from -6 to 6
- parents: int32 [4, 64], replicated, may hold values from 0 to 63, as said below
- kv_lengths: int32 [4], replicated, may hold values from 1 to 65536
- out_weight: bfloat16 [8192, 8192], P('head', 'seq'), may hold values from -0.5 to 0.5
Outputs:
- mixed: bfloat16 [256, 8192], P('head', 'seq')
The draws below stay inside these ranges and needn't reach their ends.
Inputs may be any that keep to these rules, and one draw needn't show every extreme that they name: parents[r, 0] = 0 for the root; for i >= 1, parents[r, i] < i.
All inputs are finite; a program needn't handle non-finite values.
Results may differ from the reference program's by a relative error of at most 0.0045.
Values may be sent and summed in bfloat16 or wider, within the bound.
No kernel may reach another device: no remote copies, remote signals or barrier semaphores. Data moves between devices by JAX's collectives and lax.ppermute only.
A program may use at most 64 MiB of HBM per device.

```python
import jax
import jax.numpy as jnp
from jax import lax

D = 8192
H = 64
KVH = 8
HD = 128
TREE = 64
REQS = 4
L = 65536
N_SEQ = 32


def drawn_pair(key):
    base_key = jax.random.fold_in(key, 11)
    key_query, key_draft = jax.random.split(base_key, 2)
    queries = jnp.clip(2.5 * jax.random.normal(key_query, (REQS, TREE, H, HD), jnp.float32), -15.0, 15.0)
    drafts = jnp.clip(4.0 * jax.random.normal(key_draft, (REQS, TREE, KVH, HD), jnp.float32), -16.0, 16.0)
    return (queries, drafts)


def draw_queries(key, part):
    return drawn_pair(key)[0].astype(jnp.bfloat16)


def draw_new_keys(key, part):
    return drawn_pair(key)[1].astype(jnp.bfloat16)


def draw_parents(key, part):
    tree_key = jax.random.fold_in(key, 5)
    indices = jnp.arange(TREE, dtype=jnp.int32)
    upper = jnp.maximum(indices, 1)
    raw_parents = jax.random.randint(tree_key, (REQS, TREE), 0, upper[None, :])
    return (raw_parents * (indices > 0)[None, :]).astype(jnp.int32)


def set_ends(result, rng, least, largest):
    place = [jax.random.randint(jax.random.fold_in(rng, axis), (), 0, length) for axis, length in enumerate(result.shape)]
    longest = result.shape.index(max(result.shape))
    neighbour = place[:longest] + [(place[longest] + 1) % result.shape[longest]] + place[longest + 1:]
    return result.at[tuple(place)].set(least).at[tuple(neighbour)].set(largest)


def level_of(own_key, dims, cuts, smallest, high):
    def one(dim, parts):
        heights = jax.random.uniform(jax.random.fold_in(jax.random.fold_in(own_key, 6), dim), (parts,), jnp.float32, smallest / len(cuts), high / len(cuts))
        return jnp.repeat(jnp.exp(heights), dims[dim] // parts).reshape((-1,) + (1,) * (len(dims) - dim - 1))

    gain = one(*cuts[0])
    for cut in cuts[1:]:
        gain = gain * one(*cut)
    return gain


def bell_draw(own_key, dims, width, bound, cuts=(), kind=jnp.bfloat16):
    drawn = jax.random.normal(own_key, dims, jnp.float32) * width
    if len(cuts) > 0:
        drawn = level_of(own_key, dims, cuts, -0.22, 0.18) * drawn
    return jnp.clip(drawn, min=-bound, max=bound).astype(kind)


def setup_inputs(seed: int = 0) -> dict:
    arg_keys = jax.random.split(jax.random.key(seed), 9)
    queries = draw_queries(jax.random.fold_in(arg_keys[8], 71), 0)
    new_keys = draw_new_keys(jax.random.fold_in(arg_keys[8], 71), 0)
    new_values = bell_draw(arg_keys[2], (REQS, TREE, KVH, HD), 1.0, 6.0, ((2, 8),))
    cache_keys = bell_draw(arg_keys[3], (REQS, L, KVH, HD), 1.0, 6.0, ((1, 32), (2, 8)))
    cache_values = bell_draw(arg_keys[4], (REQS, L, KVH, HD), 1.0, 6.0, ((1, 32), (2, 8)))
    parents = draw_parents(jax.random.fold_in(arg_keys[8], 71), 0)
    kv_lengths = set_ends(jax.random.randint(arg_keys[6], (REQS,), 1, L + 1), jax.random.fold_in(arg_keys[6], 1), 1, L).astype(jnp.int32)
    out_weight = bell_draw(arg_keys[7], (H * HD, D), HD ** -0.5, 0.5, ((0, 8), (1, 32)))
    return dict(queries=queries, new_keys=new_keys, new_values=new_values, cache_keys=cache_keys, cache_values=cache_values, parents=parents, kv_lengths=kv_lengths, out_weight=out_weight)


lowest = -1.0e30


def ancestors(parent_row):
    tree_size = parent_row.shape[0]
    indices = jnp.arange(tree_size, dtype=jnp.int32)
    parent_link = (parent_row[:, None] == indices[None, :]).astype(jnp.float32)
    itself = (indices[:, None] == indices[None, :]).astype(jnp.float32)
    reached = jnp.maximum(parent_link, itself)
    for repeat in range(max(1, (tree_size - 1).bit_length())):
        reached = jnp.minimum(jnp.dot(reached, reached, precision=lax.Precision.HIGHEST), 1.0)
    return reached


def block_partial(query_rows, keys, values, allowed, score_scale):
    scores = jnp.dot(query_rows, keys.T, preferred_element_type=jnp.float32) * score_scale
    scores = jnp.where(allowed, scores, lowest)
    maxima = jnp.max(scores, axis=-1)
    weights = jnp.where(allowed, jnp.exp(scores - maxima[:, None]), 0.0)
    totals = jnp.sum(weights, axis=-1)
    weighted = jnp.dot(weights.astype(jnp.bfloat16), values, preferred_element_type=jnp.float32)
    return maxima, totals, weighted


def reference(queries, new_keys, new_values, cache_keys, cache_values, parents, kv_lengths, out_weight):
    requests, tree_size, heads, head_size = queries.shape
    kv_heads = new_keys.shape[2]
    group_size = heads // kv_heads
    cache_len = cache_keys.shape[1]
    block_size = cache_len // N_SEQ
    score_scale = 1.0 / (head_size ** 0.5)
    positions = jnp.arange(cache_len, dtype=jnp.int32).reshape(N_SEQ, block_size)

    def one_request(request_items):
        query, tree_keys, tree_values, past_keys, past_values, parent_row, length = request_items
        query_rows = query.reshape(tree_size, kv_heads, group_size, head_size).transpose(1, 0, 2, 3)
        query_rows = query_rows.reshape(kv_heads, tree_size * group_size, head_size)
        tree_allowed = jnp.repeat(ancestors(parent_row), group_size, axis=0) > 0.5
        cache_allowed = positions < length

        def one_head(head_items):
            head_rows, head_tree_keys, head_tree_values, head_past_keys, head_past_values = head_items
            blocked_keys = head_past_keys.reshape(N_SEQ, block_size, head_size)
            blocked_values = head_past_values.reshape(N_SEQ, block_size, head_size)
            cache_max, cache_tot, cache_acc = jax.vmap(block_partial, in_axes=(None, 0, 0, 0, None))(
                head_rows, blocked_keys, blocked_values, cache_allowed, score_scale)
            tree_max, tree_tot, tree_acc = block_partial(head_rows, head_tree_keys, head_tree_values, tree_allowed, score_scale)
            maxima = jnp.concatenate([cache_max, tree_max[None]], axis=0)
            totals = jnp.concatenate([cache_tot, tree_tot[None]], axis=0)
            weighted = jnp.concatenate([cache_acc, tree_acc[None]], axis=0)
            overall = jnp.max(maxima, axis=0)
            factor = jnp.exp(maxima - overall[None])
            total = jnp.sum(totals * factor, axis=0)
            merged = jnp.sum(weighted * factor[:, :, None], axis=0)
            return (merged / total[:, None]).astype(jnp.bfloat16)

        attended = lax.map(one_head, (query_rows, tree_keys.transpose(1, 0, 2), tree_values.transpose(1, 0, 2),
                                      past_keys.transpose(1, 0, 2), past_values.transpose(1, 0, 2)))
        attended = attended.reshape(kv_heads, tree_size, group_size, head_size).transpose(1, 0, 2, 3)
        return attended.reshape(tree_size, heads * head_size)

    attended = lax.map(one_request, (queries, new_keys, new_values, cache_keys, cache_values, parents, kv_lengths))
    attended = attended.reshape(requests * tree_size, heads * head_size)
    return jnp.dot(attended, out_weight, preferred_element_type=jnp.float32).astype(jnp.bfloat16)
```

```python
import functools
import math

import jax
import jax.numpy as jnp
from jax import lax
from jax.experimental import pallas as pl
from jax.experimental.pallas import tpu as pltpu
from jax.sharding import PartitionSpec as P

lowest = -1e30
lanes = 128
dims_last = (((1,), (1,)), ((), ()))
dims_mid = (((1,), (0,)), ((), ()))


def iota(shape, dim):
    return lax.broadcasted_iota(jnp.int32, shape, dim)


def f32dot(a, b, dims=dims_mid):
    return lax.dot_general(a, b, dims, preferred_element_type=jnp.float32)


def regroup(count, heads):
    rows, cols = iota((count * heads, count * heads), 0), iota((count * heads, count * heads), 1)
    return (cols == (rows % count) * heads + rows // count).astype(jnp.bfloat16)


def put_stats(maxima, totals, count, heads):
    lane = iota((count, lanes), 1)
    stats = jnp.zeros((count, lanes), jnp.float32)
    high = totals.astype(jnp.bfloat16).astype(jnp.float32)
    low = totals - high
    for h in range(heads):
        part = slice(h * count, (h + 1) * count)
        stats = jnp.where(lane == h, maxima[part], stats)
        stats = jnp.where(lane == heads + h, high[part], stats)
        stats = jnp.where(lane == 2 * heads + h, low[part], stats)
    return stats


def cache_kernel(where, lengths, query, keys, values, out, scores, *, scale, chunk):
    count, heads, size = query.shape[1:]
    rows = count * heads
    block = keys.shape[1]
    valid = lengths[where[0] + pl.program_id(0)] - where[1]
    width = heads * size

    def work(masked):
        turned = f32dot(regroup(count, heads), query[0].reshape(rows, size)).astype(jnp.bfloat16)
        best = None
        for c in range(block // chunk):
            part = f32dot(turned, keys[0, c * chunk : (c + 1) * chunk], dims_last)
            if masked:
                part = jnp.where(iota((1, chunk), 1) + c * chunk < valid, part, lowest)
            scores[:, c * chunk : (c + 1) * chunk] = part
            for j in range(chunk // lanes):
                piece = part[:, j * lanes : (j + 1) * lanes]
                best = piece if best is None else jnp.maximum(best, piece)
        top = jnp.max(best, axis=1, keepdims=True) * scale
        top = top.astype(jnp.bfloat16).astype(jnp.float32)
        total = None
        for c in range(block // chunk):
            part = slice(c * chunk, (c + 1) * chunk)
            weights = jnp.exp2(scores[:, part] * scale - top).astype(jnp.bfloat16)
            wide = jnp.concatenate([values[0, part], jnp.ones((chunk, lanes), jnp.bfloat16)], axis=1)
            added = f32dot(weights, wide)
            total = added if total is None else total + added
        for h in range(heads):
            out[:, h * size : (h + 1) * size] = total[h * count : (h + 1) * count, :size].astype(out.dtype)
        stats = put_stats(jnp.broadcast_to(top, (rows, lanes)), total[:, size:], count, heads)
        out[:, width:] = stats.astype(out.dtype)

    @pl.when(valid >= block)
    def _():
        work(False)

    @pl.when((valid > 0) & (valid < block))
    def _():
        work(True)

    @pl.when(valid <= 0)
    def _():
        out[:, :width] = jnp.zeros((count, width), out.dtype)
        lane = iota((count, lanes), 1)
        out[:, width:] = jnp.where(lane < heads, lowest, 0.0).astype(out.dtype)


def cache_part(where, lengths, queries, keys, values, number, dtype, scale):
    _, count, heads, size = queries.shape
    block = keys.shape[1]
    width = heads * size + lanes
    return pl.pallas_call(
        functools.partial(cache_kernel, scale=scale, chunk=512),
        grid_spec=pltpu.PrefetchScalarGridSpec(
            num_scalar_prefetch=2,
            grid=(number,),
            in_specs=[
                pl.BlockSpec((1, count, heads, size), lambda i, w, n: (w[0] + i, 0, 0, 0)),
                pl.BlockSpec((1, block, size), lambda i, w, n: (w[0] + i, 0, 0)),
                pl.BlockSpec((1, block, size), lambda i, w, n: (w[0] + i, 0, 0)),
            ],
            out_specs=pl.BlockSpec((count, width), lambda i, w, n: (i, 0)),
            scratch_shapes=[pltpu.VMEM((count * heads, block), jnp.float32)],
        ),
        out_shape=jax.ShapeDtypeStruct((number * count, width), dtype),
        name="cache_part",
    )(where, lengths, queries, keys, values)


def join_kernel(mine, other, out, *, heads, size):
    count = mine.shape[0]
    width = heads * size
    a, b = mine[:, width:].astype(jnp.float32), other[:, width:].astype(jnp.float32)
    lane = iota((count, lanes), 1)
    top = jnp.maximum(a, b)
    fa, fb = jnp.exp2(a - top), jnp.exp2(b - top)
    fa = jnp.where(lane < heads, fa, 0.0)
    fb = jnp.where(lane < heads, fb, 0.0)
    high = a * pltpu.roll(fa, heads, 1) + b * pltpu.roll(fb, heads, 1)
    low = a * pltpu.roll(fa, 2 * heads, 1) + b * pltpu.roll(fb, 2 * heads, 1)
    total = high + pltpu.roll(low, lanes - heads, 1)
    high = total.astype(jnp.bfloat16).astype(jnp.float32)
    low = pltpu.roll(total - high, heads, 1)
    stats = jnp.where(lane < heads, top, jnp.where(lane < 2 * heads, high, low))
    out[:, width:] = stats.astype(out.dtype)
    for h in range(heads):
        part = slice(h * size, (h + 1) * size)
        sum_ = mine[:, part].astype(jnp.float32) * fa[:, h : h + 1]
        sum_ = sum_ + other[:, part].astype(jnp.float32) * fb[:, h : h + 1]
        out[:, part] = sum_.astype(out.dtype)


def join(mine, other, heads, size):
    return pl.pallas_call(
        functools.partial(join_kernel, heads=heads, size=size),
        out_shape=jax.ShapeDtypeStruct(other.shape, jnp.bfloat16),
        name="join",
    )(mine, other)


def tree_kernel(where, query, keys, values, parents, out, *, scale):
    count, heads, size = query.shape[1:]
    tree = keys.shape[1]
    width = heads * size
    parent_row = parents[pl.ds(where[0], 1), :]
    j, i = iota((tree, tree), 0), iota((tree, tree), 1)
    reached = ((parent_row == j) | (i == j)).astype(jnp.bfloat16)
    for repeat in range(max(1, (tree - 1).bit_length())):
        reached = jnp.minimum(f32dot(reached, reached), 1.0).astype(jnp.bfloat16)
    own = iota((count, tree), 1) == iota((count, tree), 0) + where[1] * count
    allowed = f32dot(own.astype(jnp.bfloat16), reached, dims_last) > 0.5
    rows = count * heads
    turned = f32dot(regroup(count, heads), query[0].reshape(rows, size)).astype(jnp.bfloat16)
    s = f32dot(turned, keys[0], dims_last).reshape(heads, count, tree)
    s = jnp.where(allowed[None], s * scale, lowest).reshape(rows, tree)
    top = jnp.max(s, axis=1, keepdims=True)
    weights = jnp.exp2(s - top).astype(jnp.bfloat16)
    wide = jnp.concatenate([values[0], jnp.ones((tree, lanes), jnp.bfloat16)], axis=1)
    total = f32dot(weights, wide)
    for h in range(heads):
        out[:, h * size : (h + 1) * size] = total[h * count : (h + 1) * count, :size]
    out[:, width:] = put_stats(jnp.broadcast_to(top, (rows, lanes)), total[:, size:], count, heads)


def tree_part(where, queries, keys, values, parents, count, scale):
    _, tree, heads, size = queries.shape
    width = heads * size + lanes
    return pl.pallas_call(
        functools.partial(tree_kernel, scale=scale),
        grid_spec=pltpu.PrefetchScalarGridSpec(
            num_scalar_prefetch=1,
            grid=(1,),
            in_specs=[
                pl.BlockSpec((1, count, heads, size), lambda i, w: (w[0], w[1], 0, 0)),
                pl.BlockSpec((1, tree, size), lambda i, w: (w[0], 0, 0)),
                pl.BlockSpec((1, tree, size), lambda i, w: (w[0], 0, 0)),
                pl.BlockSpec(parents.shape, lambda i, w: (0, 0)),
            ],
            out_specs=pl.BlockSpec((count, width), lambda i, w: (0, 0)),
        ),
        out_shape=jax.ShapeDtypeStruct((count, width), jnp.float32),
        name="tree_part",
    )(where, queries, keys, values, parents)


def finish_kernel(parts, own, out, *, heads, size):
    peers, count, _ = parts.shape
    width = heads * size
    lane = iota((count, lanes), 1)
    stats = [parts[p, :, width:].astype(jnp.float32) for p in range(peers)] + [own[:, width:]]
    top = stats[0]
    for s in stats[1:]:
        top = jnp.maximum(top, s)
    factors = [jnp.where(lane < heads, jnp.exp2(s - top), 0.0) for s in stats]
    high, low = jnp.zeros_like(top), jnp.zeros_like(top)
    for s, f in zip(stats, factors):
        high = high + s * pltpu.roll(f, heads, 1)
        low = low + s * pltpu.roll(f, 2 * heads, 1)
    total = pltpu.roll(high, lanes - heads, 1) + pltpu.roll(low, lanes - 2 * heads, 1)
    inverse = 1.0 / jnp.where(lane < heads, total, 1.0)
    for h in range(heads):
        part = slice(h * size, (h + 1) * size)
        merged = own[:, part] * factors[peers][:, h : h + 1]
        for p in range(peers):
            merged = merged + parts[p, :, part].astype(jnp.float32) * factors[p][:, h : h + 1]
        out[:, part] = (merged * inverse[:, h : h + 1]).astype(out.dtype)


def finish(parts, own, heads, size):
    return pl.pallas_call(
        functools.partial(finish_kernel, heads=heads, size=size),
        out_shape=jax.ShapeDtypeStruct((parts.shape[1], heads * size), jnp.bfloat16),
        name="finish",
    )(parts, own)


def project_kernel(which, mine, other, weight, out):
    count = mine.shape[0]
    first = pl.multiple_of(which[0] * count, count)
    second = pl.multiple_of((1 - which[0]) * count, count)
    out[pl.ds(first, count), :] = f32dot(mine[...], weight[...]).astype(out.dtype)
    out[pl.ds(second, count), :] = f32dot(other[...], weight[...]).astype(out.dtype)


def project(which, mine, other, weight):
    whole = lambda a: pl.BlockSpec(a.shape, lambda i, w: (0, 0))
    shape = (2 * mine.shape[0], weight.shape[1])
    return pl.pallas_call(
        project_kernel,
        grid_spec=pltpu.PrefetchScalarGridSpec(
            num_scalar_prefetch=1,
            grid=(1,),
            in_specs=[whole(mine), whole(other), whole(weight)],
            out_specs=pl.BlockSpec(shape, lambda i, w: (0, 0)),
        ),
        out_shape=jax.ShapeDtypeStruct(shape, jnp.bfloat16),
        name="project",
    )(which, mine, other, weight)


def body(queries, new_keys, new_values, cache_keys, cache_values, parents, kv_lengths, out_weight):
    requests, tree, heads, size = queries.shape
    peers = lax.axis_size("seq")
    head_peers = lax.axis_size("head")
    tokens = requests * tree
    block = cache_keys.shape[1]
    keys = cache_keys.reshape(requests, block, size)
    values = cache_values.reshape(requests, block, size)
    draft_keys = new_keys.reshape(requests, tree, size)
    draft_values = new_values.reshape(requests, tree, size)
    scale = math.log2(math.e) / math.sqrt(size)
    place = lax.axis_index("seq").astype(jnp.int32)
    core, chip = place % 2, place // 2
    half = requests // 2
    chips = peers // 2
    count = tokens // peers
    sibling = [(i, i ^ 1) for i in range(peers)]
    same_core = [[2 * i + c for i in range(chips)] for c in range(2)]

    def at(base):
        return jnp.stack([base, place * block]).astype(jnp.int32)

    sent = cache_part(at((1 - core) * half), kv_lengths, queries, keys, values, half, jnp.bfloat16, scale)
    arrived = lax.ppermute(sent, "seq", sibling)
    kept = cache_part(at(core * half), kv_lengths, queries, keys, values, half, jnp.float32, scale)
    pair = join(kept, arrived, heads, size)
    parts = lax.all_to_all(
        pair.reshape(chips, count, -1), "seq", 0, 0, tiled=True, axis_index_groups=same_core
    )
    first = core * (tokens // 2) + chip * count
    where = jnp.stack([first // tree, (first % tree) // count]).astype(jnp.int32)
    own = tree_part(where, queries, draft_keys, draft_values, parents, count, scale)
    share = finish(parts, own, heads, size)
    mine = lax.all_to_all(
        jnp.broadcast_to(share[None], (chips, *share.shape)),
        "seq", 0, 0, tiled=True, axis_index_groups=same_core,
    ).reshape(tokens // 2, heads * size)
    other = lax.ppermute(mine, "seq", sibling)
    partial = project(core[None], mine, other, out_weight)
    pieces = lax.all_to_all(
        partial.reshape(head_peers, tokens // head_peers, -1), "head", 0, 0, tiled=True
    )
    return pieces.astype(jnp.float32).sum(axis=0).astype(jnp.bfloat16)


def solution(mesh):
    placed = (
        P(None, None, "head", None),
        P(None, None, "head", None),
        P(None, None, "head", None),
        P(None, "seq", "head", None),
        P(None, "seq", "head", None),
        P(),
        P(),
        P("head", "seq"),
    )
    return jax.shard_map(
        body, mesh=mesh, in_specs=placed, out_specs=P("head", "seq"), check_vma=False
    )
```

```python
import functools
import math

import jax
import jax.numpy as jnp
from jax import lax
from jax.experimental import pallas as pl
from jax.experimental.pallas import tpu as pltpu
from jax.sharding import PartitionSpec as P

lowest = -1e30
lanes = 128
dims_last = (((1,), (1,)), ((), ()))
dims_mid = (((1,), (0,)), ((), ()))
on_chip = pltpu.MemorySpace.VMEM


def iota(shape, dim):
    return lax.broadcasted_iota(jnp.int32, shape, dim)


def f32dot(a, b, dims=dims_mid):
    return lax.dot_general(a, b, dims, preferred_element_type=jnp.float32)


def here(array):
    return pltpu.with_memory_space_constraint(array, on_chip)


def away(array):
    return pltpu.with_memory_space_constraint(array, pltpu.MemorySpace.HBM)


def regroup(count, heads, total, first=0):
    row, col = iota((count, heads * total), 0), iota((count, heads * total), 1)
    start = (row + first) * heads
    return jnp.concatenate([(col == start + h).astype(jnp.bfloat16) for h in range(heads)], axis=0)


def put_stats(maxima, totals, count, heads):
    lane = iota((count, lanes), 1)
    stats = jnp.zeros((count, lanes), jnp.float32)
    high = totals.astype(jnp.bfloat16).astype(jnp.float32)
    low = totals - high
    for h in range(heads):
        part = slice(h * count, (h + 1) * count)
        stats = jnp.where(lane == h, maxima[part], stats)
        stats = jnp.where(lane == heads + h, high[part], stats)
        stats = jnp.where(lane == 2 * heads + h, low[part], stats)
    return stats


def attend(turned, keys, values, valid, out, scores, count, heads, scale, chunk, ready=None):
    rows, size = turned.shape
    block = keys.shape[0]
    width = heads * size
    halves = 2
    part_rows = rows // halves
    best = [None] * halves
    for c in range(block // chunk):
        where = slice(c * chunk, (c + 1) * chunk)
        allowed = iota((1, chunk), 1) + c * chunk < valid
        for g in range(halves):
            mine = slice(g * part_rows, (g + 1) * part_rows)
            part = f32dot(turned[mine], keys[where], dims_last)
            part = jnp.where(allowed, part, lowest)
            scores[mine, where] = part
            for j in range(chunk // lanes):
                piece = part[:, j * lanes : (j + 1) * lanes]
                best[g] = piece if best[g] is None else jnp.maximum(best[g], piece)
    tops = []
    for g in range(halves):
        top = jnp.max(best[g], axis=1, keepdims=True) * scale
        tops.append(top.astype(jnp.bfloat16).astype(jnp.float32))
    if ready is not None:
        ready()
    sums = [None] * halves
    for c in range(block // chunk):
        where = slice(c * chunk, (c + 1) * chunk)
        wide = jnp.concatenate([values[where], jnp.ones((chunk, lanes), jnp.bfloat16)], axis=1)
        for g in range(halves):
            mine = slice(g * part_rows, (g + 1) * part_rows)
            weights = jnp.exp2(scores[mine, where] * scale - tops[g]).astype(jnp.bfloat16)
            added = f32dot(weights, wide)
            sums[g] = added if sums[g] is None else sums[g] + added
    some = valid > 0
    total = jnp.concatenate([jnp.where(some, s, 0.0) for s in sums], axis=0)
    top = jnp.concatenate([jnp.where(some, jnp.broadcast_to(t, (part_rows, lanes)), lowest) for t in tops], axis=0)
    for h in range(heads):
        out[:, h * size : (h + 1) * size] = total[h * count : (h + 1) * count, :size].astype(out.dtype)
    out[:, width:] = put_stats(top, total[:, size:], count, heads).astype(out.dtype)


def draft(turned, keys, values, parent_row, first, out, heads, scale):
    rows, size = turned.shape
    count, tree, width = rows // heads, keys.shape[0], heads * size
    j, i = iota((tree, tree), 0), iota((tree, tree), 1)
    reached = ((parent_row == j) | (i == j)).astype(jnp.bfloat16)
    for repeat in range(max(1, (tree - 1).bit_length())):
        reached = jnp.minimum(f32dot(reached, reached), 1.0).astype(jnp.bfloat16)
    own = iota((count, tree), 1) == iota((count, tree), 0) + first
    allowed = f32dot(own.astype(jnp.bfloat16), reached, dims_last) > 0.5
    s = f32dot(turned, keys, dims_last).reshape(heads, count, tree)
    s = jnp.where(allowed[None], s * scale, lowest).reshape(rows, tree)
    top = jnp.max(s, axis=1, keepdims=True)
    weights = jnp.exp2(s - top).astype(jnp.bfloat16)
    wide = jnp.concatenate([values, jnp.ones((tree, lanes), jnp.bfloat16)], axis=1)
    total = f32dot(weights, wide)
    for h in range(heads):
        out[:, h * size : (h + 1) * size] = total[h * count : (h + 1) * count, :size]
    out[:, width:] = put_stats(jnp.broadcast_to(top, (rows, lanes)), total[:, size:], count, heads)


def send_kernel(
    lengths, parents, queries, draft_keys, draft_values, keys, values,
    sent, own, turned, kept_keys, kept_values,
    query, left_keys, left_values, left_turned, tree_keys, tree_values, scores, sems,
    *, scale, chunk, peers,
):
    requests, tree, heads, size = queries.shape
    block = keys.shape[1]
    half = requests // 2
    count = requests * tree // peers
    place = lax.axis_index("seq")
    core, chip = lax.rem(place, 2), lax.div(place, 2)
    mine, left = core * half, (1 - core) * half
    token = chip * count
    request, first = mine + lax.div(token, tree), lax.rem(token, tree)

    copies = [
        pltpu.make_async_copy(queries, query, sems.at[0]),
        pltpu.make_async_copy(draft_keys.at[request], tree_keys, sems.at[1]),
        pltpu.make_async_copy(draft_values.at[request], tree_values, sems.at[2]),
    ]
    for r in range(half):
        copies.append(pltpu.make_async_copy(keys.at[left + r], left_keys.at[r], sems.at[3 + 2 * r]))
        copies.append(pltpu.make_async_copy(values.at[left + r], left_values.at[r], sems.at[4 + 2 * r]))
    late = 3 + 2 * half
    copies.append(pltpu.make_async_copy(keys.at[pl.ds(mine, half)], kept_keys, sems.at[late]))
    copies.append(pltpu.make_async_copy(values.at[pl.ds(mine, half)], kept_values, sems.at[late + 1]))
    for copy in copies:
        copy.start()

    spin = regroup(tree, heads, tree)
    pick = regroup(count, heads, tree, first)
    copies[0].wait()
    for r in range(half):
        left_turned[r] = f32dot(spin, query[left + r].reshape(tree * heads, size)).astype(jnp.bfloat16)
        turned[r] = f32dot(spin, query[mine + r].reshape(tree * heads, size)).astype(jnp.bfloat16)
    picked = f32dot(pick, query[request].reshape(tree * heads, size)).astype(jnp.bfloat16)
    copies[1].wait()
    copies[2].wait()
    draft(picked, tree_keys[...], tree_values[...], parents[pl.ds(request, 1), :], first, own, heads, scale)
    for r in range(half):
        copies[3 + 2 * r].wait()
        attend(
            left_turned.at[r], left_keys.at[r], left_values.at[r], lengths[left + r] - place * block,
            sent.at[pl.ds(r * tree, tree)], scores, tree, heads, scale, chunk, copies[4 + 2 * r].wait,
        )
    copies[late].wait()
    copies[late + 1].wait()


def keep_kernel(lengths, turned, keys, values, out, scores, *, scale, chunk, tree):
    half, rows, size = turned.shape
    block = keys.shape[1]
    place = lax.axis_index("seq")
    mine = lax.rem(place, 2) * half
    for r in range(half):
        attend(
            turned.at[r], keys.at[r], values.at[r], lengths[mine + r] - place * block,
            out.at[pl.ds(r * tree, tree)], scores, tree, rows // tree, scale, chunk,
        )


def cache_parts(lengths, parents, queries, draft_keys, draft_values, keys, values, peers, scale, chunk=256):
    requests, tree, heads, size = queries.shape
    block = keys.shape[1]
    half = requests // 2
    rows, width = tree * heads, heads * size + lanes
    count = requests * tree // peers
    smem, vmem, far = (pl.BlockSpec(memory_space=m) for m in (pltpu.SMEM, pltpu.VMEM, pltpu.HBM))
    scores = pltpu.VMEM((rows, block), jnp.float32)
    bf16 = jnp.bfloat16
    limit = pltpu.CompilerParams(vmem_limit_bytes=24 << 20)
    sent, own, turned, kept_keys, kept_values = pl.pallas_call(
        functools.partial(send_kernel, scale=scale, chunk=chunk, peers=peers),
        in_specs=[smem, vmem, far, far, far, far, far],
        out_specs=[vmem] * 5,
        out_shape=[
            pltpu.VMEM((half * tree, width), bf16),
            pltpu.VMEM((count, width), jnp.float32),
            pltpu.VMEM((half, rows, size), bf16),
            pltpu.VMEM((half, block, size), bf16),
            pltpu.VMEM((half, block, size), bf16),
        ],
        scratch_shapes=[
            pltpu.VMEM((requests, tree, heads, size), bf16),
            pltpu.VMEM((half, block, size), bf16),
            pltpu.VMEM((half, block, size), bf16),
            pltpu.VMEM((half, rows, size), bf16),
            pltpu.VMEM((tree, size), bf16),
            pltpu.VMEM((tree, size), bf16),
            scores,
            pltpu.SemaphoreType.DMA((5 + 2 * half,)),
        ],
        compiler_params=limit,
        name="send_part",
    )(lengths, parents, *(away(a) for a in (queries, draft_keys, draft_values, keys, values)))
    arrived = lax.ppermute(sent, "seq", [(i, i ^ 1) for i in range(peers)])
    kept = pl.pallas_call(
        functools.partial(keep_kernel, scale=scale, chunk=chunk, tree=tree),
        in_specs=[smem, vmem, vmem, vmem],
        out_specs=vmem,
        out_shape=pltpu.VMEM((half * tree, width), jnp.float32),
        scratch_shapes=[scores],
        compiler_params=limit,
        name="keep_part",
    )(lengths, here(turned), here(kept_keys), here(kept_values))
    return kept, arrived, own


def join_kernel(mine, other, out, *, heads, size):
    count = mine.shape[0]
    width = heads * size
    a, b = mine[:, width:].astype(jnp.float32), other[:, width:].astype(jnp.float32)
    lane = iota((count, lanes), 1)
    top = jnp.maximum(a, b)
    fa = jnp.where(lane < heads, jnp.exp2(a - top), 0.0)
    fb = jnp.where(lane < heads, jnp.exp2(b - top), 0.0)
    high = a * pltpu.roll(fa, heads, 1) + b * pltpu.roll(fb, heads, 1)
    low = a * pltpu.roll(fa, 2 * heads, 1) + b * pltpu.roll(fb, 2 * heads, 1)
    total = high + pltpu.roll(low, lanes - heads, 1)
    high = total.astype(jnp.bfloat16).astype(jnp.float32)
    low = pltpu.roll(total - high, heads, 1)
    stats = jnp.where(lane < heads, top, jnp.where(lane < 2 * heads, high, low))
    out[:, width:] = stats.astype(out.dtype)
    for h in range(heads):
        part = slice(h * size, (h + 1) * size)
        sum_ = mine[:, part].astype(jnp.float32) * fa[:, h : h + 1]
        sum_ = sum_ + other[:, part].astype(jnp.float32) * fb[:, h : h + 1]
        out[:, part] = sum_.astype(out.dtype)


def local_call(kernel, shape, dtype, name, *arrays):
    vmem = pl.BlockSpec(memory_space=pltpu.VMEM)
    return pl.pallas_call(
        kernel,
        in_specs=[vmem] * len(arrays),
        out_specs=vmem,
        out_shape=pltpu.VMEM(shape, dtype),
        compiler_params=pltpu.CompilerParams(vmem_limit_bytes=16 << 20),
        name=name,
    )(*(here(a) for a in arrays))


def finish_kernel(parts, own, out, *, heads, size):
    peers, count, _ = parts.shape
    width = heads * size
    lane = iota((count, lanes), 1)
    stats = [parts[p, :, width:].astype(jnp.float32) for p in range(peers)] + [own[:, width:]]
    top = stats[0]
    for s in stats[1:]:
        top = jnp.maximum(top, s)
    factors = [jnp.where(lane < heads, jnp.exp2(s - top), 0.0) for s in stats]
    high, low = jnp.zeros_like(top), jnp.zeros_like(top)
    for s, f in zip(stats, factors):
        high = high + s * pltpu.roll(f, heads, 1)
        low = low + s * pltpu.roll(f, 2 * heads, 1)
    total = pltpu.roll(high, lanes - heads, 1) + pltpu.roll(low, lanes - 2 * heads, 1)
    inverse = 1.0 / jnp.where(lane < heads, total, 1.0)
    for h in range(heads):
        part = slice(h * size, (h + 1) * size)
        merged = own[:, part] * factors[peers][:, h : h + 1]
        for p in range(peers):
            merged = merged + parts[p, :, part].astype(jnp.float32) * factors[p][:, h : h + 1]
        row = (merged * inverse[:, h : h + 1]).astype(out.dtype)
        for p in range(peers):
            out[p, :, part] = row


def project_kernel(mine, other, weight, out):
    count = mine.shape[0]
    core = lax.rem(lax.axis_index("seq"), 2)
    first = pl.multiple_of(core * count, count)
    second = pl.multiple_of((1 - core) * count, count)
    out[pl.ds(first, count), :] = f32dot(mine[...], weight[...]).astype(out.dtype)
    out[pl.ds(second, count), :] = f32dot(other[...], weight[...]).astype(out.dtype)


def body(queries, new_keys, new_values, cache_keys, cache_values, parents, kv_lengths, out_weight):
    requests, tree, heads, size = queries.shape
    peers = lax.axis_size("seq")
    head_peers = lax.axis_size("head")
    tokens = requests * tree
    block = cache_keys.shape[1]
    chips = peers // 2
    count = tokens // peers
    width = heads * size
    scale = math.log2(math.e) / math.sqrt(size)
    same_core = [[2 * i + c for i in range(chips)] for c in range(2)]
    kept, arrived, own = cache_parts(
        kv_lengths, parents, queries,
        new_keys.reshape(requests, tree, size), new_values.reshape(requests, tree, size),
        cache_keys.reshape(requests, block, size), cache_values.reshape(requests, block, size),
        peers, scale,
    )
    pair = local_call(
        functools.partial(join_kernel, heads=heads, size=size),
        (tokens // 2, width + lanes), jnp.bfloat16, "join", kept, arrived,
    )
    parts = lax.all_to_all(
        pair.reshape(chips, count, -1), "seq", 0, 0, tiled=True, axis_index_groups=same_core
    )
    share = local_call(
        functools.partial(finish_kernel, heads=heads, size=size),
        (chips, count, width), jnp.bfloat16, "finish", parts, own,
    )
    mine = lax.all_to_all(share, "seq", 0, 0, tiled=True, axis_index_groups=same_core)
    mine = mine.reshape(tokens // 2, width)
    other = lax.ppermute(mine, "seq", [(i, i ^ 1) for i in range(peers)])
    partial = local_call(
        project_kernel, (tokens, out_weight.shape[1]), jnp.bfloat16, "project", mine, other, out_weight
    )
    pieces = lax.all_to_all(
        partial.reshape(head_peers, tokens // head_peers, -1), "head", 0, 0, tiled=True
    )
    return pieces.astype(jnp.float32).sum(axis=0).astype(jnp.bfloat16)


def solution(mesh):
    placed = (
        P(None, None, "head", None),
        P(None, None, "head", None),
        P(None, None, "head", None),
        P(None, "seq", "head", None),
        P(None, "seq", "head", None),
        P(),
        P(),
        P("head", "seq"),
    )
    return jax.shard_map(
        body, mesh=mesh, in_specs=placed, out_specs=P("head", "seq"), check_vma=False
    )
```

```python
import functools
import math

import jax
import jax.numpy as jnp
from jax import lax
from jax.experimental import pallas as pl
from jax.experimental.pallas import tpu as pltpu
from jax.sharding import PartitionSpec as P

lowest = -1e30
lanes = 128
dims_last = (((1,), (1,)), ((), ()))
dims_mid = (((1,), (0,)), ((), ()))
on_chip = pltpu.MemorySpace.VMEM


def iota(shape, dim):
    return lax.broadcasted_iota(jnp.int32, shape, dim)


def f32dot(a, b, dims=dims_mid):
    return lax.dot_general(a, b, dims, preferred_element_type=jnp.float32)


def here(array):
    return pltpu.with_memory_space_constraint(array, on_chip)


def away(array):
    return pltpu.with_memory_space_constraint(array, pltpu.MemorySpace.HBM)


def owned(place, requests, tree, peers, head_peers):
    core, chip = lax.rem(place, 2), lax.div(place, 2)
    chips = peers // 4
    y, z = lax.div(chip, chips), lax.rem(chip, chips)
    tokens = requests * tree
    rows, count = tokens // head_peers, tokens // peers
    per = rows // 2 // count
    token = (core * (head_peers // 2) + lax.div(z, per)) * rows + y * (rows // 2) + lax.rem(z, per) * count
    return lax.div(token, tree), lax.rem(token, tree)


def regroup(count, heads, total, first=0):
    row, col = iota((count, heads * total), 0), iota((count, heads * total), 1)
    start = (row + first) * heads
    return jnp.concatenate([(col == start + h).astype(jnp.bfloat16) for h in range(heads)], axis=0)


def put_stats(maxima, totals, count, heads):
    lane = iota((count, lanes), 1)
    stats = jnp.zeros((count, lanes), jnp.float32)
    high = totals.astype(jnp.bfloat16).astype(jnp.float32)
    low = totals - high
    for h in range(heads):
        part = slice(h * count, (h + 1) * count)
        stats = jnp.where(lane == h, maxima[part], stats)
        stats = jnp.where(lane == heads + h, high[part], stats)
        stats = jnp.where(lane == 2 * heads + h, low[part], stats)
    return stats


def attend(turned, keys, values, valid, out, scores, count, heads, scale, chunk, ready=None):
    rows, size = turned.shape
    block = keys.shape[0]
    width = heads * size
    halves = 2
    part_rows = rows // halves
    best = [None] * halves
    for c in range(block // chunk):
        where = slice(c * chunk, (c + 1) * chunk)
        allowed = iota((1, chunk), 1) + c * chunk < valid
        for g in range(halves):
            mine = slice(g * part_rows, (g + 1) * part_rows)
            part = f32dot(turned[mine], keys[where], dims_last)
            part = jnp.where(allowed, part, lowest)
            scores[mine, where] = part
            for j in range(chunk // lanes):
                piece = part[:, j * lanes : (j + 1) * lanes]
                best[g] = piece if best[g] is None else jnp.maximum(best[g], piece)
    tops = []
    for g in range(halves):
        top = jnp.max(best[g], axis=1, keepdims=True) * scale
        tops.append(top.astype(jnp.bfloat16).astype(jnp.float32))
    if ready is not None:
        ready()
    sums = [None] * halves
    for c in range(block // chunk):
        where = slice(c * chunk, (c + 1) * chunk)
        wide = jnp.concatenate([values[where], jnp.ones((chunk, lanes), jnp.bfloat16)], axis=1)
        for g in range(halves):
            mine = slice(g * part_rows, (g + 1) * part_rows)
            weights = jnp.exp2(scores[mine, where] * scale - tops[g]).astype(jnp.bfloat16)
            added = f32dot(weights, wide)
            sums[g] = added if sums[g] is None else sums[g] + added
    some = valid > 0
    total = jnp.concatenate([jnp.where(some, s, 0.0) for s in sums], axis=0)
    top = jnp.concatenate([jnp.where(some, jnp.broadcast_to(t, (part_rows, lanes)), lowest) for t in tops], axis=0)
    for h in range(heads):
        out[:, h * size : (h + 1) * size] = total[h * count : (h + 1) * count, :size].astype(out.dtype)
    out[:, width:] = put_stats(top, total[:, size:], count, heads).astype(out.dtype)


def draft_kernel(
    parents_far, queries, draft_keys, draft_values, out, parents, query, keys, values, sems,
    *, scale, peers, head_peers,
):
    requests, tree, heads, size = queries.shape
    count, width = out.shape[0], heads * size
    rows = count * heads
    request, first = owned(lax.axis_index("seq"), requests, tree, peers, head_peers)
    first = pl.multiple_of(first, count)
    copies = [
        pltpu.make_async_copy(parents_far, parents, sems.at[0]),
        pltpu.make_async_copy(queries.at[request, pl.ds(first, count)], query, sems.at[1]),
        pltpu.make_async_copy(draft_keys.at[request], keys, sems.at[2]),
        pltpu.make_async_copy(draft_values.at[request], values, sems.at[3]),
    ]
    for copy in copies:
        copy.start()
    for copy in copies:
        copy.wait()
    turned = f32dot(regroup(count, heads, count), query[...].reshape(rows, size)).astype(jnp.bfloat16)
    parent_row = parents[pl.ds(request, 1), :]
    j, i = iota((tree, tree), 0), iota((tree, tree), 1)
    reached = ((parent_row == j) | (i == j)).astype(jnp.bfloat16)
    for repeat in range(max(1, (tree - 1).bit_length())):
        reached = jnp.minimum(f32dot(reached, reached), 1.0).astype(jnp.bfloat16)
    own = iota((count, tree), 1) == iota((count, tree), 0) + first
    allowed = f32dot(own.astype(jnp.bfloat16), reached, dims_last) > 0.5
    s = f32dot(turned, keys[...], dims_last).reshape(heads, count, tree)
    s = jnp.where(allowed[None], s * scale, lowest).reshape(rows, tree)
    top = jnp.max(s, axis=1, keepdims=True)
    weights = jnp.exp2(s - top).astype(jnp.bfloat16)
    wide = jnp.concatenate([values[...], jnp.ones((tree, lanes), jnp.bfloat16)], axis=1)
    total = f32dot(weights, wide)
    for h in range(heads):
        out[:, h * size : (h + 1) * size] = total[h * count : (h + 1) * count, :size]
    out[:, width:] = put_stats(jnp.broadcast_to(top, (rows, lanes)), total[:, size:], count, heads)


def send_kernel(
    lengths_far, queries, keys, values,
    sent, turned, kept_keys, kept_values,
    lengths, query, left_keys, left_values, left_turned, scores, sems,
    *, scale, chunk,
):
    requests, tree, heads, size = queries.shape
    block = keys.shape[1]
    half = requests // 2
    place = lax.axis_index("seq")
    core = lax.rem(place, 2)
    mine, left = core * half, (1 - core) * half

    copies = [
        pltpu.make_async_copy(lengths_far, lengths, sems.at[0]),
        pltpu.make_async_copy(queries.at[pl.ds(left, half)], query.at[pl.ds(0, half)], sems.at[1]),
        pltpu.make_async_copy(queries.at[pl.ds(mine, half)], query.at[pl.ds(half, half)], sems.at[2]),
    ]
    for r in range(half):
        copies.append(pltpu.make_async_copy(keys.at[left + r], left_keys.at[r], sems.at[3 + 2 * r]))
        copies.append(pltpu.make_async_copy(values.at[left + r], left_values.at[r], sems.at[4 + 2 * r]))
    late = 3 + 2 * half
    copies.append(pltpu.make_async_copy(keys.at[pl.ds(mine, half)], kept_keys, sems.at[late]))
    copies.append(pltpu.make_async_copy(values.at[pl.ds(mine, half)], kept_values, sems.at[late + 1]))
    for copy in copies:
        copy.start()

    spin = regroup(tree, heads, tree)
    copies[0].wait()
    copies[1].wait()
    for r in range(half):
        left_turned[r] = f32dot(spin, query[r].reshape(tree * heads, size)).astype(jnp.bfloat16)
    copies[2].wait()
    for r in range(half):
        turned[r] = f32dot(spin, query[half + r].reshape(tree * heads, size)).astype(jnp.bfloat16)
    for r in range(half):
        copies[3 + 2 * r].wait()
        attend(
            left_turned.at[r], left_keys.at[r], left_values.at[r], lengths[left + r] - place * block,
            sent.at[pl.ds(r * tree, tree)], scores, tree, heads, scale, chunk, copies[4 + 2 * r].wait,
        )
    copies[late].wait()
    copies[late + 1].wait()


def keep_kernel(lengths_far, turned, keys, values, out, lengths, scores, sem, *, scale, chunk, tree):
    copy = pltpu.make_async_copy(lengths_far, lengths, sem)
    copy.start()
    half, rows, size = turned.shape
    block = keys.shape[1]
    place = lax.axis_index("seq")
    mine = lax.rem(place, 2) * half
    copy.wait()
    for r in range(half):
        attend(
            turned.at[r], keys.at[r], values.at[r], lengths[mine + r] - place * block,
            out.at[pl.ds(r * tree, tree)], scores, tree, rows // tree, scale, chunk,
        )


def draft_part(parents, queries, draft_keys, draft_values, peers, head_peers, scale):
    requests, tree, heads, size = queries.shape
    count = requests * tree // peers
    bf16 = jnp.bfloat16
    return pl.pallas_call(
        functools.partial(draft_kernel, scale=scale, peers=peers, head_peers=head_peers),
        in_specs=[pl.BlockSpec(memory_space=pltpu.HBM)] * 4,
        out_specs=pl.BlockSpec(memory_space=pltpu.VMEM),
        out_shape=pltpu.VMEM((count, heads * size + lanes), jnp.float32),
        scratch_shapes=[
            pltpu.VMEM((requests, tree), jnp.int32),
            pltpu.VMEM((count, heads, size), bf16),
            pltpu.VMEM((tree, size), bf16),
            pltpu.VMEM((tree, size), bf16),
            pltpu.SemaphoreType.DMA((4,)),
        ],
        compiler_params=pltpu.CompilerParams(vmem_limit_bytes=8 << 20),
        name="draft_part",
    )(*(away(a) for a in (parents, queries, draft_keys, draft_values)))


def cache_parts(lengths, queries, keys, values, peers, scale, chunk=256):
    requests, tree, heads, size = queries.shape
    block = keys.shape[1]
    half = requests // 2
    rows, width = tree * heads, heads * size + lanes
    vmem, far = (pl.BlockSpec(memory_space=m) for m in (pltpu.VMEM, pltpu.HBM))
    scores = pltpu.VMEM((rows, block), jnp.float32)
    bf16 = jnp.bfloat16
    limit = pltpu.CompilerParams(vmem_limit_bytes=24 << 20)
    sent, turned, kept_keys, kept_values = pl.pallas_call(
        functools.partial(send_kernel, scale=scale, chunk=chunk),
        in_specs=[far] * 4,
        out_specs=[vmem] * 4,
        out_shape=[
            pltpu.VMEM((half * tree, width), bf16),
            pltpu.VMEM((half, rows, size), bf16),
            pltpu.VMEM((half, block, size), bf16),
            pltpu.VMEM((half, block, size), bf16),
        ],
        scratch_shapes=[
            pltpu.SMEM((requests,), jnp.int32),
            pltpu.VMEM((requests, tree, heads, size), bf16),
            pltpu.VMEM((half, block, size), bf16),
            pltpu.VMEM((half, block, size), bf16),
            pltpu.VMEM((half, rows, size), bf16),
            scores,
            pltpu.SemaphoreType.DMA((5 + 2 * half,)),
        ],
        compiler_params=limit,
        name="send_part",
    )(*(away(a) for a in (lengths, queries, keys, values)))
    arrived = lax.ppermute(sent, "seq", [(i, i ^ 1) for i in range(peers)])
    kept = pl.pallas_call(
        functools.partial(keep_kernel, scale=scale, chunk=chunk, tree=tree),
        in_specs=[far, vmem, vmem, vmem],
        out_specs=vmem,
        out_shape=pltpu.VMEM((half * tree, width), jnp.float32),
        scratch_shapes=[pltpu.SMEM((requests,), jnp.int32), scores, pltpu.SemaphoreType.DMA],
        compiler_params=limit,
        name="keep_part",
    )(away(lengths), here(turned), here(kept_keys), here(kept_values))
    return kept, arrived


def join_kernel(mine, other, out, *, heads, size, order):
    count = mine.shape[0]
    width = heads * size
    each = out.shape[1]

    def put(value, lane_slice):
        value = value.astype(out.dtype)
        for i, first in enumerate(order):
            out[i, :, lane_slice] = value[first : first + each]

    a, b = mine[:, width:].astype(jnp.float32), other[:, width:].astype(jnp.float32)
    lane = iota((count, lanes), 1)
    top = jnp.maximum(a, b)
    fa = jnp.where(lane < heads, jnp.exp2(a - top), 0.0)
    fb = jnp.where(lane < heads, jnp.exp2(b - top), 0.0)
    high = a * pltpu.roll(fa, heads, 1) + b * pltpu.roll(fb, heads, 1)
    low = a * pltpu.roll(fa, 2 * heads, 1) + b * pltpu.roll(fb, 2 * heads, 1)
    total = high + pltpu.roll(low, lanes - heads, 1)
    high = total.astype(jnp.bfloat16).astype(jnp.float32)
    low = pltpu.roll(total - high, heads, 1)
    stats = jnp.where(lane < heads, top, jnp.where(lane < 2 * heads, high, low))
    put(stats, slice(width, width + lanes))
    for h in range(heads):
        part = slice(h * size, (h + 1) * size)
        sum_ = mine[:, part].astype(jnp.float32) * fa[:, h : h + 1]
        sum_ = sum_ + other[:, part].astype(jnp.float32) * fb[:, h : h + 1]
        put(sum_, part)


def local_call(kernel, shape, dtype, name, *arrays):
    vmem = pl.BlockSpec(memory_space=pltpu.VMEM)
    return pl.pallas_call(
        kernel,
        in_specs=[vmem] * len(arrays),
        out_specs=vmem,
        out_shape=pltpu.VMEM(shape, dtype),
        compiler_params=pltpu.CompilerParams(vmem_limit_bytes=16 << 20),
        name=name,
    )(*(here(a) for a in arrays))


def finish_kernel(parts, own, out, *, heads, size):
    peers, count, _ = parts.shape
    width = heads * size
    lane = iota((count, lanes), 1)
    stats = [parts[p, :, width:].astype(jnp.float32) for p in range(peers)] + [own[:, width:]]
    top = stats[0]
    for s in stats[1:]:
        top = jnp.maximum(top, s)
    factors = [jnp.where(lane < heads, jnp.exp2(s - top), 0.0) for s in stats]
    high, low = jnp.zeros_like(top), jnp.zeros_like(top)
    for s, f in zip(stats, factors):
        high = high + s * pltpu.roll(f, heads, 1)
        low = low + s * pltpu.roll(f, 2 * heads, 1)
    total = pltpu.roll(high, lanes - heads, 1) + pltpu.roll(low, lanes - 2 * heads, 1)
    inverse = 1.0 / jnp.where(lane < heads, total, 1.0)
    for h in range(heads):
        part = slice(h * size, (h + 1) * size)
        merged = own[:, part] * factors[peers][:, h : h + 1]
        for p in range(peers):
            merged = merged + parts[p, :, part].astype(jnp.float32) * factors[p][:, h : h + 1]
        row = (merged * inverse[:, h : h + 1]).astype(out.dtype)
        for p in range(out.shape[0]):
            out[p, :, part] = row


def project_kernel(mine, other, weight, next_weight, out, *, head_peers):
    place = lax.axis_index("seq")
    core, y = lax.rem(place, 2), lax.div(place, lax.axis_size("seq") // 2)
    blocks = head_peers // 2
    rows = out.shape[1]
    for array, half in ((mine, core), (other, 1 - core)):
        for columns, at in ((weight, y), (next_weight, 1 - y)):
            part = f32dot(array[...], columns[...]).astype(out.dtype)
            out[pl.ds(at * head_peers + half * blocks, blocks)] = part.reshape(blocks, rows, -1)


def body(queries, new_keys, new_values, cache_keys, cache_values, parents, kv_lengths, out_weight):
    requests, tree, heads, size = queries.shape
    peers = lax.axis_size("seq")
    head_peers = lax.axis_size("head")
    tokens = requests * tree
    block = cache_keys.shape[1]
    chips, line = peers // 2, peers // 4
    count = tokens // peers
    width = heads * size
    rows = tokens // head_peers
    scale = math.log2(math.e) / math.sqrt(size)
    same_core = [[2 * i + c for i in range(chips)] for c in range(2)]
    same_line = [[2 * (y * line + z) + c for z in range(line)] for y in range(2) for c in range(2)]
    same_plane = [
        [(2 * (y * line + z) + c) * head_peers + h for y in range(2) for h in range(head_peers)]
        for z in range(line) for c in range(2)
    ]
    per = rows // 2 // count
    order = [(z // per) * rows + y * (rows // 2) + (z % per) * count for y in range(2) for z in range(line)]
    kept, arrived = cache_parts(
        kv_lengths, queries,
        cache_keys.reshape(requests, block, size), cache_values.reshape(requests, block, size),
        peers, scale,
    )
    next_weight = lax.ppermute(out_weight, "seq", [(i, (i + chips) % peers) for i in range(peers)])
    pair = local_call(
        functools.partial(join_kernel, heads=heads, size=size, order=order),
        (chips, count, width + lanes), jnp.bfloat16, "join", kept, arrived,
    )
    parts = lax.all_to_all(pair, "seq", 0, 0, tiled=True, axis_index_groups=same_core)
    own = draft_part(
        parents, queries,
        new_keys.reshape(requests, tree, size), new_values.reshape(requests, tree, size),
        peers, head_peers, scale,
    )
    share = local_call(
        functools.partial(finish_kernel, heads=heads, size=size),
        (line, count, width), jnp.bfloat16, "finish", parts, own,
    )
    mine = lax.all_to_all(share, "seq", 0, 0, tiled=True, axis_index_groups=same_line)
    mine = mine.reshape(line * count, width)
    other = lax.ppermute(mine, "seq", [(i, i ^ 1) for i in range(peers)])
    partial = local_call(
        functools.partial(project_kernel, head_peers=head_peers),
        (2 * head_peers, rows // 2, out_weight.shape[1]), jnp.bfloat16, "project",
        mine, other, out_weight, next_weight,
    )
    pieces = lax.all_to_all(partial, ("seq", "head"), 0, 0, tiled=True, axis_index_groups=same_plane)
    pieces = pieces.reshape(2, head_peers, rows // 2, -1).astype(jnp.float32).sum(axis=1)
    return pieces.reshape(rows, -1).astype(jnp.bfloat16)


def solution(mesh):
    placed = (
        P(None, None, "head", None),
        P(None, None, "head", None),
        P(None, None, "head", None),
        P(None, "seq", "head", None),
        P(None, "seq", "head", None),
        P(),
        P(),
        P("head", "seq"),
    )
    return jax.shard_map(
        body, mesh=mesh, in_specs=placed, out_specs=P("head", "seq"), check_vma=False
    )
```

```python
import functools
import math

import jax
import jax.numpy as jnp
from jax import lax
from jax.experimental import pallas as pl
from jax.experimental.pallas import tpu as pltpu
from jax.sharding import PartitionSpec as P


lowest = -1e30
lanes = 128
dims_last = (((1,), (1,)), ((), ()))
dims_mid = (((1,), (0,)), ((), ()))
on_chip = pltpu.MemorySpace.VMEM


def iota(shape, dim):
    return lax.broadcasted_iota(jnp.int32, shape, dim)


def f32dot(a, b, dims=dims_mid):
    return lax.dot_general(a, b, dims, preferred_element_type=jnp.float32)


def here(array):
    return pltpu.with_memory_space_constraint(array, on_chip)


def away(array):
    return pltpu.with_memory_space_constraint(array, pltpu.MemorySpace.HBM)


def owned(place, requests, tree, peers, head_peers):
    core, chip = lax.rem(place, 2), lax.div(place, 2)
    chips = peers // 4
    y, z = lax.div(chip, chips), lax.rem(chip, chips)
    tokens = requests * tree
    rows, count = tokens // head_peers, tokens // peers
    per = rows // 2 // count
    token = (core * (head_peers // 2) + lax.div(z, per)) * rows + y * (rows // 2) + lax.rem(z, per) * count
    return lax.div(token, tree), lax.rem(token, tree)


def store_partial(top, out, scratch, heads, some=None):
    acc, sums, peak = scratch
    rows, size = acc.shape
    count, width = rows // heads, heads * size
    peak[...] = jnp.broadcast_to(top, (rows, lanes))
    lane = iota((count, lanes), 1)
    stats = jnp.zeros((count, lanes), jnp.float32)

    def kept(value, other):
        return value if some is None else jnp.where(some, value, other)

    for h in range(heads):
        mine = pl.ds(h, count, heads)
        out[:, h * size : (h + 1) * size] = kept(acc[mine, :], 0.0).astype(out.dtype)
        whole = kept(sums[mine, :], 0.0)
        high = whole.astype(jnp.bfloat16).astype(jnp.float32)
        stats = jnp.where(lane == h, kept(peak[mine, :], lowest), stats)
        stats = jnp.where(lane == heads + h, high, stats)
        stats = jnp.where(lane == 2 * heads + h, whole - high, stats)
    out[:, width:] = stats.astype(out.dtype)


def score(query, keys, valid, scores, scale, chunk, halves=2):
    rows, block = scores.shape
    part_rows = rows // halves
    best = [None] * halves
    for c in range(block // chunk):
        where = slice(c * chunk, (c + 1) * chunk)
        allowed = iota((1, chunk), 1) + c * chunk < valid
        for g in range(halves):
            mine = slice(g * part_rows, (g + 1) * part_rows)
            part = f32dot(query[mine], keys[where], dims_last)
            part = jnp.where(allowed, part, lowest)
            scores[mine, where] = part
            for j in range(chunk // lanes):
                piece = part[:, j * lanes : (j + 1) * lanes]
                best[g] = piece if best[g] is None else jnp.maximum(best[g], piece)
    tops = []
    for g in range(halves):
        top = jnp.max(best[g], axis=1, keepdims=True) * scale
        tops.append(top.astype(jnp.bfloat16).astype(jnp.float32))
    return tops


def gather_values(scores, values, tops, scratch, scale, chunk):
    acc, sums, _ = scratch
    rows, block = scores.shape
    size = acc.shape[1]
    halves = len(tops)
    part_rows = rows // halves
    added_up = [None] * halves
    for c in range(block // chunk):
        where = slice(c * chunk, (c + 1) * chunk)
        wide = jnp.concatenate([values[where], jnp.ones((chunk, lanes), jnp.bfloat16)], axis=1)
        for g in range(halves):
            mine = slice(g * part_rows, (g + 1) * part_rows)
            weights = jnp.exp2(scores[mine, where] * scale - tops[g]).astype(jnp.bfloat16)
            added = f32dot(weights, wide)
            added_up[g] = added if added_up[g] is None else added_up[g] + added
    for g in range(halves):
        mine = slice(g * part_rows, (g + 1) * part_rows)
        acc[mine, :] = added_up[g][:, :size]
        sums[mine, :] = added_up[g][:, size:]


def attend(
    query, keys, values, valids, out, scratch, tree, heads, scale, chunk, beside=None
):
    scores, *partial = scratch
    number = query.shape[0]
    tops = []
    for r in range(number):
        if r == number - 1 and beside is not None:
            beside()
        tops.append(score(query.at[r], keys.at[r], valids[r], scores.at[r], scale, chunk))
    for r in range(number):
        gather_values(scores.at[r], values.at[r], tops[r], [a.at[r] for a in partial], scale, chunk)
    for r in range(number):
        top = jnp.concatenate(tops[r], axis=0)
        store_partial(top, out.at[pl.ds(r * tree, tree)], [a.at[r] for a in partial], heads, valids[r] > 0)


def draft(query, keys, values, parent_row, first, out, partial, heads, scale):
    rows, size = query.shape
    tree = keys.shape[0]
    count = rows // heads
    acc, sums, _ = partial
    j, i = iota((tree, tree), 0), iota((tree, tree), 1)
    reached = ((parent_row == j) | (i == j)).astype(jnp.bfloat16)
    for _ in range(max(1, (tree - 1).bit_length())):
        reached = jnp.minimum(f32dot(reached, reached), 1.0).astype(jnp.bfloat16)
    own = iota((count, tree), 1) == iota((count, tree), 0) + first
    allowed = f32dot(own.astype(jnp.bfloat16), reached, dims_last) > 0.5
    s = f32dot(query[...], keys[...], dims_last).reshape(count, heads, tree)
    s = jnp.where(allowed[:, None, :], s * scale, lowest).reshape(rows, tree)
    top = jnp.max(s, axis=1, keepdims=True)
    weights = jnp.exp2(s - top).astype(jnp.bfloat16)
    wide = jnp.concatenate([values[...], jnp.ones((tree, lanes), jnp.bfloat16)], axis=1)
    total = f32dot(weights, wide)
    acc[...] = total[:, :size]
    sums[...] = total[:, size:]
    store_partial(top, out, partial, heads)


def send_kernel(
    lengths_far, parents_far, queries, draft_keys, draft_values, keys, values,
    sent, own, lengths, kept_query, kept_keys, kept_values,
    parents, own_query, tree_keys, tree_values, own_acc, own_sums, own_peak,
    query, left_keys, left_values, scores, acc, sums, peak, sems,
    *, scale, chunk, tree, heads, peers, head_peers,
):
    block = keys.shape[1]
    requests = queries.shape[0]
    half = requests // 2
    own_rows = own_query.shape[0]
    place = lax.axis_index("seq")
    core = lax.rem(place, 2)
    mine, left = core * half, (1 - core) * half
    request, first = owned(place, requests, tree, peers, head_peers)
    own_first = pl.multiple_of(first * heads, own_rows)

    pairs = [(lengths_far, lengths), (queries.at[pl.ds(left, half)], query)]
    pairs += [(keys.at[left], left_keys.at[0]), (parents_far, parents)]
    pairs += [(queries.at[request, pl.ds(own_first, own_rows)], own_query)]
    pairs += [(draft_keys.at[request], tree_keys), (draft_values.at[request], tree_values)]
    pairs += [(keys.at[left + r], left_keys.at[r]) for r in range(1, half)]
    pairs += [(values.at[left + r], left_values.at[r]) for r in range(half)]
    late = len(pairs)
    pairs += [(queries.at[pl.ds(mine, half)], kept_query)]
    pairs += [(keys.at[pl.ds(mine, half)], kept_keys), (values.at[pl.ds(mine, half)], kept_values)]
    copies = [pltpu.make_async_copy(a, b, sems.at[i]) for i, (a, b) in enumerate(pairs)]
    for copy in copies:
        copy.start()
    early = 3
    for copy in copies[:early]:
        copy.wait()

    def rest():
        for copy in copies[early:late]:
            copy.wait()
        draft(
            own_query, tree_keys, tree_values, parents[pl.ds(request, 1), :], first, own,
            (own_acc, own_sums, own_peak), heads, scale,
        )

    attend(
        query, left_keys, left_values, [lengths[left + r] - place * block for r in range(half)],
        sent, (scores, acc, sums, peak), tree, heads, scale, chunk,
        rest,
    )
    for copy in copies[late:]:
        copy.wait()


def keep_kernel(lengths, query, keys, values, out, scores, acc, sums, peak, *, scale, chunk, tree, heads):
    half = query.shape[0]
    block = keys.shape[1]
    place = lax.axis_index("seq")
    mine = lax.rem(place, 2) * half
    attend(
        query, keys, values, [lengths[mine + r] - place * block for r in range(half)],
        out, (scores, acc, sums, peak), tree, heads, scale, chunk,
    )


def partial_scratch(*shape):
    return [pltpu.VMEM((*shape, n), jnp.float32) for n in (lanes, lanes, lanes)]


def cache_parts(lengths, parents, queries, draft_keys, draft_values, keys, values, heads, peers, head_peers, scale):
    requests, rows, size = queries.shape
    block, tree = keys.shape[1], draft_keys.shape[1]
    half = requests // 2
    count = requests * tree // peers
    width = heads * size + lanes
    vmem, far, smem = (pl.BlockSpec(memory_space=m) for m in (pltpu.VMEM, pltpu.HBM, pltpu.SMEM))
    working = [pltpu.VMEM((half, rows, block), jnp.float32), *partial_scratch(half, rows)]
    bf16 = jnp.bfloat16
    limit = pltpu.CompilerParams(vmem_limit_bytes=32 << 20)
    settings = dict(scale=scale, chunk=256, tree=tree, heads=heads)
    sent, own, known, kept_query, kept_keys, kept_values = pl.pallas_call(
        functools.partial(send_kernel, peers=peers, head_peers=head_peers, **settings),
        in_specs=[far] * 7,
        out_specs=[vmem, vmem, smem, vmem, vmem, vmem],
        out_shape=[
            pltpu.VMEM((half * tree, width), bf16),
            pltpu.VMEM((count, width), jnp.float32),
            pltpu.SMEM((requests,), jnp.int32),
            pltpu.VMEM((half, rows, size), bf16),
            pltpu.VMEM((half, block, size), bf16),
            pltpu.VMEM((half, block, size), bf16),
        ],
        scratch_shapes=[
            pltpu.VMEM((requests, tree), jnp.int32),
            pltpu.VMEM((count * heads, size), bf16),
            pltpu.VMEM((tree, size), bf16),
            pltpu.VMEM((tree, size), bf16),
            *partial_scratch(count * heads),
            pltpu.VMEM((half, rows, size), bf16),
            pltpu.VMEM((half, block, size), bf16),
            pltpu.VMEM((half, block, size), bf16),
            *working,
            pltpu.SemaphoreType.DMA((9 + 2 * half,)),
        ],
        compiler_params=limit,
        name="send_part",
    )(*(away(a) for a in (lengths, parents, queries, draft_keys, draft_values, keys, values)))
    arrived = lax.ppermute(sent, "seq", [(i, i ^ 1) for i in range(peers)])
    kept = pl.pallas_call(
        functools.partial(keep_kernel, **settings),
        in_specs=[smem, vmem, vmem, vmem],
        out_specs=vmem,
        out_shape=pltpu.VMEM((half * tree, width), jnp.float32),
        scratch_shapes=working,
        compiler_params=limit,
        name="keep_part",
    )(
        pltpu.with_memory_space_constraint(known, pltpu.MemorySpace.SMEM),
        here(kept_query), here(kept_keys), here(kept_values),
    )
    return kept, arrived, own


def join_kernel(mine, other, out, *, heads, size, order):
    count = mine.shape[0]
    width = heads * size
    each = out.shape[1]

    def put(value, lane_slice):
        value = value.astype(out.dtype)
        for i, first in enumerate(order):
            out[i, :, lane_slice] = value[first : first + each]

    a, b = mine[:, width:].astype(jnp.float32), other[:, width:].astype(jnp.float32)
    lane = iota((count, lanes), 1)
    top = jnp.maximum(a, b)
    fa = jnp.where(lane < heads, jnp.exp2(a - top), 0.0)
    fb = jnp.where(lane < heads, jnp.exp2(b - top), 0.0)
    high = a * pltpu.roll(fa, heads, 1) + b * pltpu.roll(fb, heads, 1)
    low = a * pltpu.roll(fa, 2 * heads, 1) + b * pltpu.roll(fb, 2 * heads, 1)
    total = high + pltpu.roll(low, lanes - heads, 1)
    high = total.astype(jnp.bfloat16).astype(jnp.float32)
    low = pltpu.roll(total - high, heads, 1)
    stats = jnp.where(lane < heads, top, jnp.where(lane < 2 * heads, high, low))
    put(stats, slice(width, width + lanes))
    for h in range(heads):
        part = slice(h * size, (h + 1) * size)
        sum_ = mine[:, part].astype(jnp.float32) * fa[:, h : h + 1]
        sum_ = sum_ + other[:, part].astype(jnp.float32) * fb[:, h : h + 1]
        put(sum_, part)


def local_call(kernel, shape, dtype, *arrays):
    vmem = pl.BlockSpec(memory_space=pltpu.VMEM)
    return pl.pallas_call(
        kernel,
        in_specs=[vmem] * len(arrays),
        out_specs=vmem,
        out_shape=pltpu.VMEM(shape, dtype),
        compiler_params=pltpu.CompilerParams(vmem_limit_bytes=16 << 20),
    )(*(here(a) for a in arrays))


def finish_kernel(parts, own, out, *, heads, size):
    peers, count, _ = parts.shape
    width = heads * size
    lane = iota((count, lanes), 1)
    stats = [parts[p, :, width:].astype(jnp.float32) for p in range(peers)] + [own[:, width:]]
    top = stats[0]
    for s in stats[1:]:
        top = jnp.maximum(top, s)
    factors = [jnp.where(lane < heads, jnp.exp2(s - top), 0.0) for s in stats]
    high, low = jnp.zeros_like(top), jnp.zeros_like(top)
    for s, f in zip(stats, factors):
        high = high + s * pltpu.roll(f, heads, 1)
        low = low + s * pltpu.roll(f, 2 * heads, 1)
    total = pltpu.roll(high, lanes - heads, 1) + pltpu.roll(low, lanes - 2 * heads, 1)
    inverse = 1.0 / jnp.where(lane < heads, total, 1.0)
    for h in range(heads):
        part = slice(h * size, (h + 1) * size)
        merged = own[:, part] * factors[peers][:, h : h + 1]
        for p in range(peers):
            merged = merged + parts[p, :, part].astype(jnp.float32) * factors[p][:, h : h + 1]
        row = (merged * inverse[:, h : h + 1]).astype(out.dtype)
        for p in range(out.shape[0]):
            out[p, :, part] = row


def project_kernel(mine, other, weight, next_weight, out, *, head_peers, block_order):
    place = lax.axis_index("seq")
    core, y = lax.rem(place, 2), lax.div(place, lax.axis_size("seq") // 2)
    blocks = head_peers // 2
    rows = out.shape[1]
    for array, half in ((mine, core), (other, 1 - core)):
        for columns, at in ((weight, y), (next_weight, 1 - y)):
            part = f32dot(array[...], columns[...]).astype(out.dtype)
            last = at * head_peers + head_peers - 1 - half * blocks
            for k, b in enumerate(block_order):
                out[last - b] = part[k * rows : (k + 1) * rows]


def body(queries, new_keys, new_values, cache_keys, cache_values, parents, kv_lengths, out_weight):
    requests, tree, heads, size = queries.shape
    peers = lax.axis_size("seq")
    head_peers = lax.axis_size("head")
    tokens = requests * tree
    block = cache_keys.shape[1]
    chips, line = peers // 2, peers // 4
    count = tokens // peers
    width = heads * size
    rows = tokens // head_peers
    scale = math.log2(math.e) / math.sqrt(size)
    per = rows // 2 // count
    line_order = [*range(line // 2, line), *range(line // 2)]
    chip_order = [(y, z) for y in (1, 0) for z in line_order]
    plane_order = [(y, h) for y in range(2) for h in reversed(range(head_peers))]
    same_core = [[2 * (y * line + z) + c for y, z in chip_order] for c in range(2)]
    same_line = [[2 * (y * line + z) + c for z in line_order] for y in range(2) for c in range(2)]
    same_plane = [
        [(2 * (y * line + z) + c) * head_peers + h for y, h in plane_order]
        for z in range(line) for c in range(2)
    ]
    order = [z // per * rows + y * (rows // 2) + z % per * count for y, z in chip_order]
    block_order = [z // per for z in line_order[::per]]
    query_rows = queries.reshape(requests, tree * heads, size)
    kept, arrived, own = cache_parts(
        kv_lengths, parents, query_rows,
        new_keys.reshape(requests, tree, size), new_values.reshape(requests, tree, size),
        cache_keys.reshape(requests, block, size), cache_values.reshape(requests, block, size),
        heads, peers, head_peers, scale,
    )
    next_weight = lax.ppermute(out_weight, "seq", [(i, (i + chips) % peers) for i in range(peers)])
    pair = local_call(
        functools.partial(join_kernel, heads=heads, size=size, order=order),
        (chips, count, width + lanes), jnp.bfloat16, kept, arrived,
    )
    parts = lax.all_to_all(pair, "seq", 0, 0, tiled=True, axis_index_groups=same_core)
    share = local_call(
        functools.partial(finish_kernel, heads=heads, size=size),
        (line, count, width), jnp.bfloat16, parts, own,
    )
    mine = lax.all_to_all(share, "seq", 0, 0, tiled=True, axis_index_groups=same_line)
    mine = mine.reshape(line * count, width)
    other = lax.ppermute(mine, "seq", [(i, i ^ 1) for i in range(peers)])
    partial = local_call(
        functools.partial(project_kernel, head_peers=head_peers, block_order=block_order),
        (2 * head_peers, rows // 2, out_weight.shape[1]), jnp.bfloat16,
        mine, other, out_weight, next_weight,
    )
    pieces = lax.all_to_all(partial, ("seq", "head"), 0, 0, tiled=True, axis_index_groups=same_plane)
    pieces = pieces.reshape(2, head_peers, rows // 2, -1).astype(jnp.float32).sum(axis=1)
    return pieces.reshape(rows, -1).astype(jnp.bfloat16)


def solution(mesh):
    placed = (
        P(None, None, "head", None),
        P(None, None, "head", None),
        P(None, None, "head", None),
        P(None, "seq", "head", None),
        P(None, "seq", "head", None),
        P(),
        P(),
        P("head", "seq"),
    )

    return jax.shard_map(body, mesh=mesh, in_specs=placed, out_specs=P("head", "seq"), check_vma=False)
```

```python
import functools
import math

import jax
import jax.numpy as jnp
from jax import lax
from jax.experimental import pallas as pl
from jax.experimental.pallas import tpu as pltpu
from jax.sharding import PartitionSpec as P


lowest = -1e30
lanes = 128
dims_last = (((1,), (1,)), ((), ()))
dims_mid = (((1,), (0,)), ((), ()))
on_chip = pltpu.MemorySpace.VMEM


def iota(shape, dim):
    return lax.broadcasted_iota(jnp.int32, shape, dim)


def f32dot(a, b, dims=dims_mid):
    return lax.dot_general(a, b, dims, preferred_element_type=jnp.float32)


def here(array):
    return pltpu.with_memory_space_constraint(array, on_chip)


def away(array):
    return pltpu.with_memory_space_constraint(array, pltpu.MemorySpace.HBM)


def owned(place, requests, tree, peers, head_peers):
    core, chip = lax.rem(place, 2), lax.div(place, 2)
    chips = peers // 4
    y, z = lax.div(chip, chips), lax.rem(chip, chips)
    tokens = requests * tree
    rows, count = tokens // head_peers, tokens // peers
    per = rows // 2 // count
    token = (core * (head_peers // 2) + lax.div(z, per)) * rows + y * (rows // 2) + lax.rem(z, per) * count
    return lax.div(token, tree), lax.rem(token, tree)


def store_partial(top, out, scratch, heads, some=None):
    acc, sums, peak = scratch
    rows, size = acc.shape
    count, width = rows // heads, heads * size
    peak[...] = jnp.broadcast_to(top, (rows, lanes))
    lane = iota((count, lanes), 1)
    stats = jnp.zeros((count, lanes), jnp.float32)

    def kept(value, other):
        return value if some is None else jnp.where(some, value, other)

    for h in range(heads):
        mine = pl.ds(h, count, heads)
        out[:, h * size : (h + 1) * size] = kept(acc[mine, :], 0.0).astype(out.dtype)
        whole = kept(sums[mine, :], 0.0)
        high = whole.astype(jnp.bfloat16).astype(jnp.float32)
        stats = jnp.where(lane == h, kept(peak[mine, :], lowest), stats)
        stats = jnp.where(lane == heads + h, high, stats)
        stats = jnp.where(lane == 2 * heads + h, whole - high, stats)
    out[:, width:] = stats.astype(out.dtype)


def score(query, keys, valid, scores, scale, chunk, halves=2):
    rows, block = scores.shape
    part_rows = rows // halves
    best = [None] * halves
    for c in range(block // chunk):
        where = slice(c * chunk, (c + 1) * chunk)
        allowed = iota((1, chunk), 1) + c * chunk < valid
        for g in range(halves):
            mine = slice(g * part_rows, (g + 1) * part_rows)
            part = f32dot(query[mine], keys[where], dims_last)
            part = jnp.where(allowed, part, lowest)
            scores[mine, where] = part
            for j in range(chunk // lanes):
                piece = part[:, j * lanes : (j + 1) * lanes]
                best[g] = piece if best[g] is None else jnp.maximum(best[g], piece)
    tops = []
    for g in range(halves):
        top = jnp.max(best[g], axis=1, keepdims=True) * scale
        tops.append(top.astype(jnp.bfloat16).astype(jnp.float32))
    return tops


def gather_values(scores, values, tops, scratch, scale, chunk):
    acc, sums, _ = scratch
    rows, block = scores.shape
    size = acc.shape[1]
    halves = len(tops)
    part_rows = rows // halves
    added_up = [None] * halves
    for c in range(block // chunk):
        where = slice(c * chunk, (c + 1) * chunk)
        wide = jnp.concatenate([values[where], jnp.ones((chunk, lanes), jnp.bfloat16)], axis=1)
        for g in range(halves):
            mine = slice(g * part_rows, (g + 1) * part_rows)
            weights = jnp.exp2(scores[mine, where] * scale - tops[g]).astype(jnp.bfloat16)
            added = f32dot(weights, wide)
            added_up[g] = added if added_up[g] is None else added_up[g] + added
    for g in range(halves):
        mine = slice(g * part_rows, (g + 1) * part_rows)
        acc[mine, :] = added_up[g][:, :size]
        sums[mine, :] = added_up[g][:, size:]


def attend(
    query, keys, values, valids, out, scratch, tree, heads, scale, chunk, beside=None, after=None
):
    scores, *partial = scratch
    number = query.shape[0]
    tops = []
    for r in range(number):
        if r == number - 1 and beside is not None:
            beside()
        tops.append(score(query.at[r], keys.at[r], valids[r], scores.at[r], scale, chunk))
    if after is not None:
        after()
    for r in range(number):
        gather_values(scores.at[r], values.at[r], tops[r], [a.at[r] for a in partial], scale, chunk)
    for r in range(number):
        top = jnp.concatenate(tops[r], axis=0)
        store_partial(top, out.at[pl.ds(r * tree, tree)], [a.at[r] for a in partial], heads, valids[r] > 0)


def ancestors(parent_row, first, count):
    tree = parent_row.shape[1]
    j, i = iota((tree, tree), 0), iota((tree, tree), 1)
    reached = ((parent_row == j) | (i == j)).astype(jnp.bfloat16)
    for _ in range(max(1, (tree - 1).bit_length())):
        reached = jnp.minimum(f32dot(reached, reached), 1.0).astype(jnp.bfloat16)
    own = iota((count, tree), 1) == iota((count, tree), 0) + first
    return f32dot(own.astype(jnp.bfloat16), reached, dims_last)


def draft(query, keys, values, seen, out, partial, heads, scale):
    rows, size = query.shape
    tree = keys.shape[0]
    count = rows // heads
    acc, sums, _ = partial
    allowed = seen > 0.5
    s = f32dot(query[...], keys[...], dims_last).reshape(count, heads, tree)
    s = jnp.where(allowed[:, None, :], s * scale, lowest).reshape(rows, tree)
    top = jnp.max(s, axis=1, keepdims=True)
    weights = jnp.exp2(s - top).astype(jnp.bfloat16)
    wide = jnp.concatenate([values[...], jnp.ones((tree, lanes), jnp.bfloat16)], axis=1)
    total = f32dot(weights, wide)
    acc[...] = total[:, :size]
    sums[...] = total[:, size:]
    store_partial(top, out, partial, heads)


def send_kernel(
    lengths_far, parents_far, queries, draft_keys, draft_values, keys, values,
    sent, own, lengths, kept_query, kept_keys, kept_values,
    parents, own_query, tree_keys, tree_values, own_acc, own_sums, own_peak,
    query, left_keys, left_values, scores, acc, sums, peak, sems,
    *, scale, chunk, tree, heads, peers, head_peers,
):
    block = keys.shape[1]
    requests = queries.shape[0]
    half = requests // 2
    own_rows = own_query.shape[0]
    place = lax.axis_index("seq")
    core = lax.rem(place, 2)
    mine, left = core * half, (1 - core) * half
    request, first = owned(place, requests, tree, peers, head_peers)
    own_first = pl.multiple_of(first * heads, own_rows)

    pairs = [(parents_far, parents), (lengths_far, lengths)]
    pairs += [(queries.at[pl.ds(left, half)], query), (keys.at[left], left_keys.at[0])]
    early = len(pairs)
    pairs += [(queries.at[request, pl.ds(own_first, own_rows)], own_query)]
    pairs += [(draft_keys.at[request], tree_keys), (draft_values.at[request], tree_values)]
    pairs += [(keys.at[left + r], left_keys.at[r]) for r in range(1, half)]
    pairs += [(values.at[left + r], left_values.at[r]) for r in range(half)]
    late = len(pairs)
    pairs += [(queries.at[pl.ds(mine, half)], kept_query)]
    pairs += [(keys.at[pl.ds(mine, half)], kept_keys), (values.at[pl.ds(mine, half)], kept_values)]
    copies = [pltpu.make_async_copy(a, b, sems.at[i]) for i, (a, b) in enumerate(pairs)]
    for copy in copies[:late]:
        copy.start()
    copies[0].wait()
    seen = ancestors(parents[pl.ds(request, 1), :], first, own_rows // heads)
    for copy in copies[1:early]:
        copy.wait()
    for copy in copies[late:]:
        copy.start()

    def rest():
        for copy in copies[early : late - half]:
            copy.wait()

    def last():
        for copy in copies[late - half : late]:
            copy.wait()
        draft(own_query, tree_keys, tree_values, seen, own, (own_acc, own_sums, own_peak), heads, scale)

    attend(
        query, left_keys, left_values, [lengths[left + r] - place * block for r in range(half)],
        sent, (scores, acc, sums, peak), tree, heads, scale, chunk,
        rest, last,
    )
    for copy in copies[late:]:
        copy.wait()


def keep_kernel(lengths, query, keys, values, out, scores, acc, sums, peak, *, scale, chunk, tree, heads):
    half = query.shape[0]
    block = keys.shape[1]
    place = lax.axis_index("seq")
    mine = lax.rem(place, 2) * half
    attend(
        query, keys, values, [lengths[mine + r] - place * block for r in range(half)],
        out, (scores, acc, sums, peak), tree, heads, scale, chunk,
    )


def partial_scratch(*shape):
    return [pltpu.VMEM((*shape, n), jnp.float32) for n in (lanes, lanes, lanes)]


def cache_parts(lengths, parents, queries, draft_keys, draft_values, keys, values, heads, peers, head_peers, scale):
    requests, rows, size = queries.shape
    block, tree = keys.shape[1], draft_keys.shape[1]
    half = requests // 2
    count = requests * tree // peers
    width = heads * size + lanes
    vmem, far, smem = (pl.BlockSpec(memory_space=m) for m in (pltpu.VMEM, pltpu.HBM, pltpu.SMEM))
    working = [pltpu.VMEM((half, rows, block), jnp.float32), *partial_scratch(half, rows)]
    bf16 = jnp.bfloat16
    limit = pltpu.CompilerParams(vmem_limit_bytes=32 << 20)
    settings = dict(scale=scale, chunk=256, tree=tree, heads=heads)
    sent, own, known, kept_query, kept_keys, kept_values = pl.pallas_call(
        functools.partial(send_kernel, peers=peers, head_peers=head_peers, **settings),
        in_specs=[far] * 7,
        out_specs=[vmem, vmem, smem, vmem, vmem, vmem],
        out_shape=[
            pltpu.VMEM((half * tree, width), bf16),
            pltpu.VMEM((count, width), jnp.float32),
            pltpu.SMEM((requests,), jnp.int32),
            pltpu.VMEM((half, rows, size), bf16),
            pltpu.VMEM((half, block, size), bf16),
            pltpu.VMEM((half, block, size), bf16),
        ],
        scratch_shapes=[
            pltpu.VMEM((requests, tree), jnp.int32),
            pltpu.VMEM((count * heads, size), bf16),
            pltpu.VMEM((tree, size), bf16),
            pltpu.VMEM((tree, size), bf16),
            *partial_scratch(count * heads),
            pltpu.VMEM((half, rows, size), bf16),
            pltpu.VMEM((half, block, size), bf16),
            pltpu.VMEM((half, block, size), bf16),
            *working,
            pltpu.SemaphoreType.DMA((9 + 2 * half,)),
        ],
        compiler_params=limit,
        name="send_part",
    )(*(away(a) for a in (lengths, parents, queries, draft_keys, draft_values, keys, values)))
    arrived = lax.ppermute(sent, "seq", [(i, i ^ 1) for i in range(peers)])
    kept = pl.pallas_call(
        functools.partial(keep_kernel, **settings),
        in_specs=[smem, vmem, vmem, vmem],
        out_specs=vmem,
        out_shape=pltpu.VMEM((half * tree, width), jnp.float32),
        scratch_shapes=working,
        compiler_params=limit,
        name="keep_part",
    )(
        pltpu.with_memory_space_constraint(known, pltpu.MemorySpace.SMEM),
        here(kept_query), here(kept_keys), here(kept_values),
    )
    return kept, arrived, own


def join_kernel(mine, other, out, *, heads, size, order):
    count = mine.shape[0]
    width = heads * size
    each = out.shape[1]

    def put(value, lane_slice):
        value = value.astype(out.dtype)
        for i, first in enumerate(order):
            out[i, :, lane_slice] = value[first : first + each]

    a, b = mine[:, width:].astype(jnp.float32), other[:, width:].astype(jnp.float32)
    lane = iota((count, lanes), 1)
    top = jnp.maximum(a, b)
    fa = jnp.where(lane < heads, jnp.exp2(a - top), 0.0)
    fb = jnp.where(lane < heads, jnp.exp2(b - top), 0.0)
    high = a * pltpu.roll(fa, heads, 1) + b * pltpu.roll(fb, heads, 1)
    low = a * pltpu.roll(fa, 2 * heads, 1) + b * pltpu.roll(fb, 2 * heads, 1)
    total = high + pltpu.roll(low, lanes - heads, 1)
    high = total.astype(jnp.bfloat16).astype(jnp.float32)
    low = pltpu.roll(total - high, heads, 1)
    stats = jnp.where(lane < heads, top, jnp.where(lane < 2 * heads, high, low))
    put(stats, slice(width, width + lanes))
    for h in range(heads):
        part = slice(h * size, (h + 1) * size)
        sum_ = mine[:, part].astype(jnp.float32) * fa[:, h : h + 1]
        sum_ = sum_ + other[:, part].astype(jnp.float32) * fb[:, h : h + 1]
        put(sum_, part)


def local_call(kernel, shape, dtype, *arrays):
    vmem = pl.BlockSpec(memory_space=pltpu.VMEM)
    return pl.pallas_call(
        kernel,
        in_specs=[vmem] * len(arrays),
        out_specs=vmem,
        out_shape=pltpu.VMEM(shape, dtype),
        compiler_params=pltpu.CompilerParams(vmem_limit_bytes=16 << 20),
    )(*(here(a) for a in arrays))


def finish_kernel(parts, own, out, *, heads, size):
    peers, count, _ = parts.shape
    width = heads * size
    lane = iota((count, lanes), 1)
    stats = [parts[p, :, width:].astype(jnp.float32) for p in range(peers)] + [own[:, width:]]
    top = stats[0]
    for s in stats[1:]:
        top = jnp.maximum(top, s)
    factors = [jnp.where(lane < heads, jnp.exp2(s - top), 0.0) for s in stats]
    high, low = jnp.zeros_like(top), jnp.zeros_like(top)
    for s, f in zip(stats, factors):
        high = high + s * pltpu.roll(f, heads, 1)
        low = low + s * pltpu.roll(f, 2 * heads, 1)
    total = pltpu.roll(high, lanes - heads, 1) + pltpu.roll(low, lanes - 2 * heads, 1)
    inverse = 1.0 / jnp.where(lane < heads, total, 1.0)
    for h in range(heads):
        part = slice(h * size, (h + 1) * size)
        merged = own[:, part] * factors[peers][:, h : h + 1]
        for p in range(peers):
            merged = merged + parts[p, :, part].astype(jnp.float32) * factors[p][:, h : h + 1]
        row = (merged * inverse[:, h : h + 1]).astype(out.dtype)
        for p in range(out.shape[0]):
            out[p, :, part] = row


def project_kernel(mine, other, weight, next_weight, out, *, head_peers, block_order):
    place = lax.axis_index("seq")
    core, y = lax.rem(place, 2), lax.div(place, lax.axis_size("seq") // 2)
    blocks = head_peers // 2
    rows = out.shape[1]
    for array, half in ((mine, core), (other, 1 - core)):
        for columns, at in ((weight, y), (next_weight, 1 - y)):
            part = f32dot(array[...], columns[...]).astype(out.dtype)
            last = at * head_peers + head_peers - 1 - half * blocks
            for k, b in enumerate(block_order):
                out[last - b] = part[k * rows : (k + 1) * rows]


def body(queries, new_keys, new_values, cache_keys, cache_values, parents, kv_lengths, out_weight):
    requests, tree, heads, size = queries.shape
    peers = lax.axis_size("seq")
    head_peers = lax.axis_size("head")
    tokens = requests * tree
    block = cache_keys.shape[1]
    chips, line = peers // 2, peers // 4
    count = tokens // peers
    width = heads * size
    rows = tokens // head_peers
    scale = math.log2(math.e) / math.sqrt(size)
    per = rows // 2 // count
    line_order = [*range(line // 2, line), *range(line // 2)]
    chip_order = [(y, z) for y in range(2) for z in line_order]
    plane_order = [(y, h) for y in range(2) for h in reversed(range(head_peers))]
    same_core = [[2 * (y * line + z) + c for y, z in chip_order] for c in range(2)]
    same_line = [[2 * (y * line + z) + c for z in line_order] for y in range(2) for c in range(2)]
    same_plane = [
        [(2 * (y * line + z) + c) * head_peers + h for y, h in plane_order]
        for z in range(line) for c in range(2)
    ]
    order = [z // per * rows + y * (rows // 2) + z % per * count for y, z in chip_order]
    block_order = [z // per for z in line_order[::per]]
    query_rows = queries.reshape(requests, tree * heads, size)
    kept, arrived, own = cache_parts(
        kv_lengths, parents, query_rows,
        new_keys.reshape(requests, tree, size), new_values.reshape(requests, tree, size),
        cache_keys.reshape(requests, block, size), cache_values.reshape(requests, block, size),
        heads, peers, head_peers, scale,
    )
    next_weight = lax.ppermute(out_weight, "seq", [(i, (i + chips) % peers) for i in range(peers)])
    pair = local_call(
        functools.partial(join_kernel, heads=heads, size=size, order=order),
        (chips, count, width + lanes), jnp.bfloat16, kept, arrived,
    )
    parts = lax.all_to_all(pair, "seq", 0, 0, tiled=True, axis_index_groups=same_core)
    share = local_call(
        functools.partial(finish_kernel, heads=heads, size=size),
        (line, count, width), jnp.bfloat16, parts, own,
    )
    mine = lax.all_to_all(share, "seq", 0, 0, tiled=True, axis_index_groups=same_line)
    mine = mine.reshape(line * count, width)
    other = lax.ppermute(mine, "seq", [(i, i ^ 1) for i in range(peers)])
    partial = local_call(
        functools.partial(project_kernel, head_peers=head_peers, block_order=block_order),
        (2 * head_peers, rows // 2, out_weight.shape[1]), jnp.bfloat16,
        mine, other, out_weight, next_weight,
    )
    pieces = lax.all_to_all(partial, ("seq", "head"), 0, 0, tiled=True, axis_index_groups=same_plane)
    pieces = pieces.reshape(2, head_peers, rows // 2, -1).astype(jnp.float32).sum(axis=1)
    return pieces.reshape(rows, -1).astype(jnp.bfloat16)


def solution(mesh):
    placed = (
        P(None, None, "head", None),
        P(None, None, "head", None),
        P(None, None, "head", None),
        P(None, "seq", "head", None),
        P(None, "seq", "head", None),
        P(),
        P(),
        P("head", "seq"),
    )

    return jax.shard_map(body, mesh=mesh, in_specs=placed, out_specs=P("head", "seq"), check_vma=False)
```
